32 devices in a mesh: lat: 4 (over y, x), lon: 4 (over z), lev: 2 (over core).
Axes of the slice: x: 2, y: 2, z: 4, core: 2. Of those that a mesh axis runs over, the one named last changes fastest.
Arguments:
- field_values: float32 [16, 256, 192, 128], P('lat', 'lon', 'lev'), may hold values from 0.2 to 1.8
- crowding: float32 [16, 256, 192, 128], P('lat', 'lon', 'lev'), may hold values from 0.5 to 2
Outputs:
- field_values_end: float32 [16, 256, 192, 128], P('lat', 'lon', 'lev')
The draws below stay inside these ranges and needn't reach their ends.
All inputs are finite; a program needn't handle non-finite values.
Results may differ from the reference program's by a relative error of at most 0.00002.
Values sent between devices are 32-bit elements; how exact they have to be, the bound alone decides.
A program may use at most 384 MiB of HBM per device.

```python
import jax
import jax.numpy as jnp
from jax import lax

GRID_J = 16
GRID_I = 256
GRID_K = 192
LEVELS = 128
STEPS = 3


def level_of(stream_key, shape, pieces, least, top_value):
    def one(axis_at, shards_of):
        heights = jax.random.uniform(jax.random.fold_in(jax.random.fold_in(stream_key, 6), axis_at), (shards_of,), jnp.float32, least / len(pieces), top_value / len(pieces))
        return jnp.repeat(jnp.exp(heights), shape[axis_at] // shards_of).reshape((-1,) + (1,) * (len(shape) - axis_at - 1))

    level = one(*pieces[0])
    for cut in pieces[1:]:
        level = level * one(*cut)
    return level


def setup_inputs(seed: int = 0) -> dict:
    arg_keys = jax.random.split(jax.random.key(seed), 3)
    field_values = jnp.clip(0.2 + 1.5999999 * jax.random.uniform(arg_keys[0], (GRID_J, GRID_I, GRID_K, LEVELS), jnp.float32) ** level_of(arg_keys[0], (GRID_J, GRID_I, GRID_K, LEVELS), ((0, 4), (1, 4), (2, 2)), -0.2, 0.2), 0.2, 1.8)
    crowding = jnp.clip(0.5 + 1.5 * jax.random.uniform(arg_keys[1], (GRID_J, GRID_I, GRID_K, LEVELS), jnp.float32) ** level_of(arg_keys[1], (GRID_J, GRID_I, GRID_K, LEVELS), ((0, 4), (1, 4), (2, 2)), -0.2, 0.2), 0.5, 2.0)
    return {"field_values": field_values, "crowding": crowding}


def without_rim(values, dims):
    for dim in dims:
        values = lax.slice_in_dim(values, 1, values.shape[dim] - 1, axis=dim)
    return values


def shifted_cells(values, dim, start, dims):
    others = [other for other in dims if other != dim]
    values = without_rim(values, others)
    return lax.slice_in_dim(values, start, start + values.shape[dim] - 2, axis=dim)


def march_step(padded, crowding):
    middle = without_rim(padded, (0, 1, 2))
    lower = [shifted_cells(padded, dim, 0, (0, 1, 2)) for dim in (0, 1, 2)]
    upper = [shifted_cells(padded, dim, 2, (0, 1, 2)) for dim in (0, 1, 2)]
    spread = lower[0] + upper[0] + lower[1] + upper[1] + lower[2] + upper[2] - 6.0 * middle
    return middle + 0.1 * spread + 0.2 * middle * (1.0 - middle * crowding)


def reference(field_values, crowding):
    for step in range(STEPS):
        field_values = march_step(jnp.pad(field_values, ((1, 1), (1, 1), (1, 1), (0, 0)), mode="wrap"), crowding)
    return field_values
```

```python
import functools
import math

import jax
import jax.numpy as jnp
from jax import lax
from jax.experimental import pallas as pl
from jax.experimental.pallas import tpu as pltpu
from jax.sharding import PartitionSpec as P

STEPS = 3
CHUNK_ROWS = 8
WINDOW = 5
TAIL_CHUNKS = 2
PIECE_ROWS = 4
MESH = pl.DeviceIdType.MESH
AXES = ("lat", "lon", "lev")


def neighbours(sizes, axis):
    count, me = sizes[AXES.index(axis)], lax.axis_index(axis)
    return lax.rem(me + count - 1, count), lax.rem(me + 1, count)


def is_late(sizes):
    return lax.axis_index("lev") == sizes[AXES.index("lev")] - 1


def signal(sizes, axis, semaphore):
    for target in neighbours(sizes, axis):
        pl.semaphore_signal(semaphore, inc=1, device_id={axis: target}, device_id_type=MESH)


def enter(sizes, ready):
    barrier = pltpu.get_barrier_semaphore()
    second = {axis: lax.rem(lax.axis_index(axis), 2) == parity
              for axis, parity in (("lon", 1), ("lev", 0))}
    signal(sizes, "lat", barrier)
    pl.semaphore_wait(barrier, 2 + sum(2 * second[axis].astype(jnp.int32) for axis in second))

    def answer():
        for axis in second:
            pl.when(jnp.logical_not(second[axis]))(lambda: signal(sizes, axis, barrier))
            pl.when(second[axis])(lambda: signal(sizes, axis, ready.at[AXES.index(axis)]))

    def await_answer(axis):
        pl.when(jnp.logical_not(second[axis]))(
            lambda: pl.semaphore_wait(ready.at[AXES.index(axis)], 2))

    return answer, await_answer


def enter_together(sizes, axes):
    barrier = pltpu.get_barrier_semaphore()
    for axis in axes:
        signal(sizes, axis, barrier)
    pl.semaphore_wait(barrier, 2 * len(axes))


def march_kernel(sizes, shape, rows, tail, f_in, c_in, odd, even, crowd, jh, kh, kf,
                 load_sems, j_send, j_recv, i_send, i_recv, k_send, k_recv, ready):
    J, I, K, L = shape
    chunks = I // rows
    near = {axis: neighbours(sizes, axis) for axis in AXES}
    last_chunks = chunks - jnp.where(is_late(sizes), tail, 0) if tail else chunks

    if any(size % 2 for size in sizes[1:]):
        enter_together(sizes, AXES)
        answer, await_answer = lambda: None, lambda axis: None
    else:
        answer, await_answer = enter(sizes, ready)

    fields = (even, odd)

    def remote(source, target, send, recv, axis, side):
        return pltpu.make_async_remote_copy(
            src_ref=source, dst_ref=target, send_sem=send, recv_sem=recv,
            device_id={axis: near[axis][side]}, device_id_type=MESH)

    def j_copy(step, side, chunk):
        j = (J - 1) * side
        if step == 0:
            source = f_in.at[j, pl.ds(chunk * rows, rows)]
        else:
            source = fields[step % 2].at[j, pl.ds(1 + chunk * rows, rows)]
        return remote(source, jh.at[step, 1 - side, pl.ds(chunk * rows, rows)],
                      j_send.at[step, side, chunk], j_recv.at[step, 1 - side, chunk], "lat", side)

    def i_copy(step, side):
        if step == 0:
            source = f_in.at[:, (I - 1) * side]
        else:
            source = fields[step % 2].at[:, 1 + (I - 1) * side]
        return remote(source, fields[step % 2].at[:, (I + 1) * (1 - side)],
                      i_send.at[step, side], i_recv.at[step, 1 - side], "lon", side)

    def k_copy(step, side):
        return remote(kf.at[step, side], kh.at[step, 1 - side],
                      k_send.at[step, side], k_recv.at[step, 1 - side], "lev", side)

    window = min(WINDOW, chunks - 1 - tail)

    @pl.loop(0, window)
    def _(chunk):
        for side in (0, 1):
            j_copy(0, side, chunk).start()

    answer()
    load_f = pltpu.make_async_copy(f_in, even.at[:, pl.ds(1, I)], load_sems.at[0])
    load_c = pltpu.make_async_copy(c_in, crowd, load_sems.at[1])
    load_f.start()
    load_c.start()
    await_answer("lon")
    for side in (0, 1):
        i_copy(0, side).start()
    load_f.wait()

    @pl.loop(0, I)
    def _(i):
        for j in range(J):
            kf[0, 0, j, pl.ds(i, 1), :] = even[j, i + 1, 0:1, :]
            kf[0, 1, j, pl.ds(i, 1), :] = even[j, i + 1, K - 1:K, :]

    load_c.wait()
    await_answer("lev")
    for side in (0, 1):
        k_copy(0, side).start()

    at_k = lax.broadcasted_iota(jnp.int32, (K, L), 0)

    for step in range(STEPS):
        source, target = fields[step % 2], fields[(step + 1) % 2]
        last = step == STEPS - 1

        def update(i, j, below, above):
            middle = source[j, i + 1]
            total = source[j, i] + source[j, i + 2]
            if below is not None:
                total += below
            if above is not None:
                total += above
            total += jnp.where(at_k == 0, kh[step, 0, j, pl.ds(i, 1), :],
                               pltpu.roll(middle, 1, 0))
            total += jnp.where(at_k == K - 1, kh[step, 1, j, pl.ds(i, 1), :],
                               pltpu.roll(middle, K - 1, 0))
            return middle * (0.6 - 0.2 * (middle * crowd[j, i])) + 0.1 * total

        for side in (0, 1):
            i_copy(step, side).wait_recv()
            k_copy(step, side).wait_recv()
            if step >= 1:
                i_copy(step - 1, side).wait_send()

        if last:
            @pl.loop(window, last_chunks)
            def _(chunk):
                for side in (0, 1):
                    j_copy(step, side, chunk).start()

            @pl.loop(0, I)
            def _(i):
                for j in range(J):
                    target[j, i + 1] = update(
                        i, j, None if j == 0 else source[j - 1, i + 1],
                        None if j == J - 1 else source[j + 1, i + 1])

            @pl.loop(0, last_chunks)
            def _(chunk):
                for side in (0, 1):
                    j_copy(step, side, chunk).wait_recv()
                    j_copy(step, side, chunk).wait_send()

                @pl.loop(0, rows)
                def _(row):
                    i = chunk * rows + row
                    for side in (0, 1):
                        j = (J - 1) * side
                        target[j, i + 1] = target[j, i + 1] + 0.1 * jh[step, side, i]
        else:
            @pl.loop(0, chunks)
            def _(chunk):
                for side in (0, 1):
                    j_copy(step, side, chunk).wait_recv()
                    j_copy(step, side, chunk).wait_send()

                @pl.when(chunk + window < chunks)
                def _():
                    for side in (0, 1):
                        j_copy(step, side, chunk + window).start()

                @pl.when(chunk + window >= chunks)
                def _():
                    for side in (0, 1):
                        j_copy(step + 1, side, chunk + window - chunks).start()

                @pl.loop(0, rows)
                def _(row):
                    i = chunk * rows + row
                    for j in range(J):
                        new = update(
                            i, j, jh[step, 0, i] if j == 0 else source[j - 1, i + 1],
                            jh[step, 1, i] if j == J - 1 else source[j + 1, i + 1])
                        target[j, i + 1] = new
                        kf[step + 1, 0, j, pl.ds(i, 1), :] = new[0:1]
                        kf[step + 1, 1, j, pl.ds(i, 1), :] = new[K - 1:K]

            for side in (0, 1):
                i_copy(step + 1, side).start()
                k_copy(step + 1, side).start()

    for side in (0, 1):
        i_copy(STEPS - 1, side).wait_send()
        for step in range(STEPS):
            k_copy(step, side).wait_send()


def write_kernel(shape, held, out, done, sems):
    J, I = shape[:2]
    copies = [pltpu.make_async_copy(held.at[j, pl.ds(1, I)], out.at[j], sems.at[j])
              for j in range(J)]
    for copy in copies:
        copy.start()
    done[...] = jnp.zeros_like(done)
    for copy in copies:
        copy.wait()


def tail_kernel(sizes, shape, length, rows, done, held, even, fresh, halo, sends, recvs):
    J, I = shape[:2]
    first = I - length
    late = is_late(sizes)

    @pl.when(late)
    def _():
        enter_together(sizes, ("lat",))
        near = neighbours(sizes, "lat")

        def j_copy(side, piece):
            return pltpu.make_async_remote_copy(
                src_ref=even.at[(J - 1) * side, pl.ds(1 + first + piece * rows, rows)],
                dst_ref=halo.at[1 - side, pl.ds(piece * rows, rows)],
                send_sem=sends.at[side, piece], recv_sem=recvs.at[1 - side, piece],
                device_id={"lat": near[side]}, device_id_type=MESH)

        @pl.loop(0, length // rows)
        def _(piece):
            for side in (0, 1):
                j_copy(side, piece).start()

        @pl.loop(0, length // rows)
        def _(piece):
            for side in (0, 1):
                j_copy(side, piece).wait_recv()

            @pl.loop(0, rows)
            def _(row):
                i = piece * rows + row
                for side in (0, 1):
                    fresh[side, i] = held[(J - 1) * side, 1 + first + i] + 0.1 * halo[side, i]

        @pl.loop(0, length // rows)
        def _(piece):
            for side in (0, 1):
                j_copy(side, piece).wait_send()

    @pl.when(jnp.logical_not(late))
    def _():
        @pl.loop(0, length)
        def _(i):
            for side in (0, 1):
                fresh[side, i] = held[(J - 1) * side, 1 + first + i]


def patch_kernel(shape, length, fresh, before, out, sems):
    J, I = shape[:2]
    copies = [pltpu.make_async_copy(fresh.at[side], out.at[(J - 1) * side, pl.ds(I - length, length)],
                                    sems.at[side]) for side in (0, 1)]
    for copy in copies:
        copy.start()
    for copy in copies:
        copy.wait()


def local(sizes, field_values, crowding):
    J, I, K, L = shape = field_values.shape
    rows = math.gcd(I, CHUNK_ROWS)
    chunks = I // rows
    tail = TAIL_CHUNKS if J >= 2 and chunks > TAIL_CHUNKS + 1 else 0
    length = tail * rows
    dtype = field_values.dtype
    DMA = pltpu.SemaphoreType.DMA
    VMEM = pltpu.VMEM
    whole = VMEM((J, I + 2, K, L), dtype)
    in_vmem, anywhere = pl.BlockSpec(memory_space=VMEM), pl.BlockSpec(memory_space=pl.ANY)
    fields = pl.pallas_call(
        functools.partial(march_kernel, sizes, shape, rows, tail),
        out_shape=(whole,) * (2 if tail else 1),
        in_specs=[anywhere] * 2,
        out_specs=(in_vmem,) * (2 if tail else 1),
        scratch_shapes=[whole] * (0 if tail else 1) + [
            VMEM(shape, dtype),
            VMEM((STEPS, 2, I, K, L), dtype),
            VMEM((STEPS, 2, J, I, L), dtype),
            VMEM((STEPS, 2, J, I, L), dtype),
            DMA((2,)),
            DMA((STEPS, 2, chunks)),
            DMA((STEPS, 2, chunks)),
            DMA((STEPS, 2)),
            DMA((STEPS, 2)),
            DMA((STEPS, 2)),
            DMA((STEPS, 2)),
            pltpu.SemaphoreType.REGULAR((len(AXES),)),
        ],
        compiler_params=pltpu.CompilerParams(
            collective_id=0, has_side_effects=True, vmem_limit_bytes=(36 if tail else 50) * 1024 * 1024),
    )(field_values, crowding)
    fields = [pltpu.with_memory_space_constraint(field, VMEM) for field in fields]
    out, done = pl.pallas_call(
        functools.partial(write_kernel, shape),
        out_shape=(jax.ShapeDtypeStruct(shape, dtype), VMEM((8, 128), dtype)),
        in_specs=[in_vmem],
        out_specs=(anywhere, in_vmem),
        scratch_shapes=[DMA((J,))],
        compiler_params=pltpu.CompilerParams(vmem_limit_bytes=1024 * 1024),
    )(fields[0])
    if not tail:
        return out
    piece = math.gcd(length, PIECE_ROWS)
    outer = VMEM((2, length, K, L), dtype)
    fresh = pl.pallas_call(
        functools.partial(tail_kernel, sizes, shape, length, piece),
        out_shape=outer,
        in_specs=[in_vmem] * 3,
        out_specs=in_vmem,
        scratch_shapes=[outer, DMA((2, length // piece)), DMA((2, length // piece))],
        compiler_params=pltpu.CompilerParams(
            collective_id=1, has_side_effects=True, vmem_limit_bytes=4 * 1024 * 1024),
    )(pltpu.with_memory_space_constraint(done, VMEM), *fields)
    return pl.pallas_call(
        functools.partial(patch_kernel, shape, length),
        out_shape=jax.ShapeDtypeStruct(shape, dtype),
        in_specs=[in_vmem, anywhere],
        out_specs=anywhere,
        scratch_shapes=[DMA((2,))],
        input_output_aliases={1: 0},
        compiler_params=pltpu.CompilerParams(vmem_limit_bytes=1024 * 1024),
    )(pltpu.with_memory_space_constraint(fresh, VMEM), out)


def solution(mesh):
    spec = P("lat", "lon", "lev", None)
    sizes = tuple(mesh.shape[axis] for axis in AXES)
    return jax.shard_map(
        functools.partial(local, sizes), mesh=mesh, in_specs=(spec, spec), out_specs=spec,
        check_vma=False,
    )
```

```python
import functools
import math

import jax
import jax.numpy as jnp
from jax import lax
from jax.experimental import pallas as pl
from jax.experimental.pallas import tpu as pltpu
from jax.sharding import PartitionSpec as P

STEPS = 3
CHUNK_ROWS = 8
WINDOW = 5
TAIL_CHUNKS = 2
PIECE_ROWS = 4
MESH = pl.DeviceIdType.MESH
AXES = ("lat", "lon", "lev")


def neighbours(sizes, axis):
    count, me = sizes[AXES.index(axis)], lax.axis_index(axis)
    return lax.rem(me + count - 1, count), lax.rem(me + 1, count)


def is_late(sizes):
    return lax.axis_index("lev") == sizes[AXES.index("lev")] - 1


def signal(sizes, axis, semaphore):
    for target in neighbours(sizes, axis):
        pl.semaphore_signal(semaphore, inc=1, device_id={axis: target}, device_id_type=MESH)


def enter(sizes, ready):
    barrier = pltpu.get_barrier_semaphore()
    odd = lax.rem(lax.axis_index("lat"), 2) == 1
    follow = lax.rem(lax.axis_index("lev"), 2) == 0
    before, after = neighbours(sizes, "lat")

    def tell(semaphore, **target):
        pl.semaphore_signal(semaphore, inc=1, device_id=target, device_id_type=MESH)

    @pl.when(odd)
    def _():
        tell(barrier, lat=before)

    @pl.when(jnp.logical_not(odd))
    def _():
        tell(barrier, lat=after)
        tell(barrier, lat=before)

    pl.when(follow)(lambda: signal(sizes, "lon", barrier))
    pl.semaphore_wait(barrier, 1 + odd.astype(jnp.int32) + 8 * follow.astype(jnp.int32))

    @pl.when(odd)
    def _():
        tell(ready.at[0], lat=after)

    def answer():
        pl.when(follow)(lambda: signal(sizes, "lev", ready.at[1]))

        @pl.when(jnp.logical_not(follow))
        def _():
            signal(sizes, "lev", barrier)
            for lon in neighbours(sizes, "lon"):
                for lev in neighbours(sizes, "lev"):
                    tell(barrier, lon=lon, lev=lev)

    def await_lat():
        pl.when(jnp.logical_not(odd))(lambda: pl.semaphore_wait(ready.at[0], 1))

    def await_rest():
        pl.when(jnp.logical_not(follow))(lambda: pl.semaphore_wait(ready.at[1], 2))

    return answer, await_lat, await_rest


def enter_together(sizes, axes):
    barrier = pltpu.get_barrier_semaphore()
    for axis in axes:
        signal(sizes, axis, barrier)
    pl.semaphore_wait(barrier, 2 * len(axes))


def march_kernel(sizes, shape, rows, tail, f_in, c_in, odd, even, crowd, jh, kh, kf,
                 load_sems, j_send, j_recv, i_send, i_recv, k_send, k_recv, ready):
    J, I, K, L = shape
    chunks = I // rows
    near = {axis: neighbours(sizes, axis) for axis in AXES}
    last_chunks = chunks - jnp.where(is_late(sizes), tail, 0) if tail else chunks

    if sizes[0] % 2 or sizes[2] % 2:
        enter_together(sizes, AXES)
        answer = await_lat = await_rest = lambda: None
    else:
        answer, await_lat, await_rest = enter(sizes, ready)

    fields = (even, odd)

    def remote(source, target, send, recv, axis, side):
        return pltpu.make_async_remote_copy(
            src_ref=source, dst_ref=target, send_sem=send, recv_sem=recv,
            device_id={axis: near[axis][side]}, device_id_type=MESH)

    def j_copy(step, side, chunk):
        j = (J - 1) * side
        if step == 0:
            source = f_in.at[j, pl.ds(chunk * rows, rows)]
        else:
            source = fields[step % 2].at[j, pl.ds(1 + chunk * rows, rows)]
        return remote(source, jh.at[step, 1 - side, pl.ds(chunk * rows, rows)],
                      j_send.at[step, side, chunk], j_recv.at[step, 1 - side, chunk], "lat", side)

    def i_copy(step, side):
        if step == 0:
            source = f_in.at[:, (I - 1) * side]
        else:
            source = fields[step % 2].at[:, 1 + (I - 1) * side]
        return remote(source, fields[step % 2].at[:, (I + 1) * (1 - side)],
                      i_send.at[step, side], i_recv.at[step, 1 - side], "lon", side)

    def k_copy(step, side):
        return remote(kf.at[step, side], kh.at[step, 1 - side],
                      k_send.at[step, side], k_recv.at[step, 1 - side], "lev", side)

    window = min(WINDOW, chunks - 1 - tail)

    j_copy(0, 1, 0).start()
    answer()
    await_lat()
    j_copy(0, 0, 0).start()

    @pl.loop(1, window)
    def _(chunk):
        for side in (0, 1):
            j_copy(0, side, chunk).start()

    load_f = pltpu.make_async_copy(f_in, even.at[:, pl.ds(1, I)], load_sems.at[0])
    load_c = pltpu.make_async_copy(c_in, crowd, load_sems.at[1])
    load_f.start()
    load_c.start()
    await_rest()
    for side in (0, 1):
        i_copy(0, side).start()
    load_f.wait()

    @pl.loop(0, I)
    def _(i):
        for j in range(J):
            kf[0, 0, j, pl.ds(i, 1), :] = even[j, i + 1, 0:1, :]
            kf[0, 1, j, pl.ds(i, 1), :] = even[j, i + 1, K - 1:K, :]

    load_c.wait()
    for side in (0, 1):
        k_copy(0, side).start()

    at_k = lax.broadcasted_iota(jnp.int32, (K, L), 0)

    for step in range(STEPS):
        source, target = fields[step % 2], fields[(step + 1) % 2]
        last = step == STEPS - 1

        def update(i, j, below, above):
            middle = source[j, i + 1]
            total = source[j, i] + source[j, i + 2]
            if below is not None:
                total += below
            if above is not None:
                total += above
            total += jnp.where(at_k == 0, kh[step, 0, j, pl.ds(i, 1), :],
                               pltpu.roll(middle, 1, 0))
            total += jnp.where(at_k == K - 1, kh[step, 1, j, pl.ds(i, 1), :],
                               pltpu.roll(middle, K - 1, 0))
            return middle * (0.6 - 0.2 * (middle * crowd[j, i])) + 0.1 * total

        for side in (0, 1):
            i_copy(step, side).wait_recv()
            k_copy(step, side).wait_recv()
            if step >= 1:
                i_copy(step - 1, side).wait_send()

        if last:
            @pl.loop(window, last_chunks)
            def _(chunk):
                for side in (0, 1):
                    j_copy(step, side, chunk).start()

            @pl.loop(0, I)
            def _(i):
                for j in range(J):
                    target[j, i + 1] = update(
                        i, j, None if j == 0 else source[j - 1, i + 1],
                        None if j == J - 1 else source[j + 1, i + 1])

            @pl.loop(0, last_chunks)
            def _(chunk):
                for side in (0, 1):
                    j_copy(step, side, chunk).wait_recv()
                    j_copy(step, side, chunk).wait_send()

                @pl.loop(0, rows)
                def _(row):
                    i = chunk * rows + row
                    for side in (0, 1):
                        j = (J - 1) * side
                        target[j, i + 1] = target[j, i + 1] + 0.1 * jh[step, side, i]
        else:
            @pl.loop(0, chunks)
            def _(chunk):
                for side in (0, 1):
                    j_copy(step, side, chunk).wait_recv()
                    j_copy(step, side, chunk).wait_send()

                @pl.when(chunk + window < chunks)
                def _():
                    for side in (0, 1):
                        j_copy(step, side, chunk + window).start()

                @pl.when(chunk + window >= chunks)
                def _():
                    for side in (0, 1):
                        j_copy(step + 1, side, chunk + window - chunks).start()

                @pl.loop(0, rows)
                def _(row):
                    i = chunk * rows + row
                    for j in range(J):
                        new = update(
                            i, j, jh[step, 0, i] if j == 0 else source[j - 1, i + 1],
                            jh[step, 1, i] if j == J - 1 else source[j + 1, i + 1])
                        target[j, i + 1] = new
                        kf[step + 1, 0, j, pl.ds(i, 1), :] = new[0:1]
                        kf[step + 1, 1, j, pl.ds(i, 1), :] = new[K - 1:K]

            for side in (0, 1):
                i_copy(step + 1, side).start()
                k_copy(step + 1, side).start()

    for side in (0, 1):
        i_copy(STEPS - 1, side).wait_send()
        for step in range(STEPS):
            k_copy(step, side).wait_send()


def write_kernel(shape, held, out, done, sems):
    J, I = shape[:2]
    copies = [pltpu.make_async_copy(held.at[j, pl.ds(1, I)], out.at[j], sems.at[j])
              for j in range(J)]
    for copy in copies:
        copy.start()
    done[...] = jnp.zeros_like(done)
    for copy in copies:
        copy.wait()


def tail_kernel(sizes, shape, length, rows, done, held, even, fresh, halo, sends, recvs):
    J, I = shape[:2]
    first = I - length

    @pl.when(is_late(sizes))
    def _():
        enter_together(sizes, ("lat",))
        near = neighbours(sizes, "lat")

        def j_copy(side, piece):
            return pltpu.make_async_remote_copy(
                src_ref=even.at[(J - 1) * side, pl.ds(1 + first + piece * rows, rows)],
                dst_ref=halo.at[1 - side, pl.ds(piece * rows, rows)],
                send_sem=sends.at[side, piece], recv_sem=recvs.at[1 - side, piece],
                device_id={"lat": near[side]}, device_id_type=MESH)

        odd = lax.rem(lax.axis_index("lat"), 2) == 1

        @pl.loop(0, length // rows)
        def _(piece):
            pl.when(odd)(lambda: j_copy(1, piece).start())
            j_copy(0, piece).start()
            pl.when(jnp.logical_not(odd))(lambda: j_copy(1, piece).start())

        @pl.loop(0, length // rows)
        def _(piece):
            for side in (0, 1):
                j_copy(side, piece).wait_recv()

            @pl.loop(0, rows)
            def _(row):
                i = piece * rows + row
                for side in (0, 1):
                    fresh[side, i] = held[(J - 1) * side, 1 + first + i] + 0.1 * halo[side, i]

        @pl.loop(0, length // rows)
        def _(piece):
            for side in (0, 1):
                j_copy(side, piece).wait_send()


def patch_kernel(sizes, shape, length, fresh, before, out, sems):
    J, I = shape[:2]

    @pl.when(is_late(sizes))
    def _():
        copies = [
            pltpu.make_async_copy(
                fresh.at[side], out.at[(J - 1) * side, pl.ds(I - length, length)], sems.at[side])
            for side in (0, 1)]
        for copy in copies:
            copy.start()
        for copy in copies:
            copy.wait()


def local(sizes, field_values, crowding):
    J, I, K, L = shape = field_values.shape
    rows = math.gcd(I, CHUNK_ROWS)
    chunks = I // rows
    tail = TAIL_CHUNKS if J >= 2 and chunks > TAIL_CHUNKS + 1 else 0
    length = tail * rows
    dtype = field_values.dtype
    DMA = pltpu.SemaphoreType.DMA
    VMEM = pltpu.VMEM
    whole = VMEM((J, I + 2, K, L), dtype)
    in_vmem, anywhere = pl.BlockSpec(memory_space=VMEM), pl.BlockSpec(memory_space=pl.ANY)
    fields = pl.pallas_call(
        functools.partial(march_kernel, sizes, shape, rows, tail),
        out_shape=(whole,) * (2 if tail else 1),
        in_specs=[anywhere] * 2,
        out_specs=(in_vmem,) * (2 if tail else 1),
        scratch_shapes=[whole] * (0 if tail else 1) + [
            VMEM(shape, dtype),
            VMEM((STEPS, 2, I, K, L), dtype),
            VMEM((STEPS, 2, J, I, L), dtype),
            VMEM((STEPS, 2, J, I, L), dtype),
            DMA((2,)),
            DMA((STEPS, 2, chunks)),
            DMA((STEPS, 2, chunks)),
            DMA((STEPS, 2)),
            DMA((STEPS, 2)),
            DMA((STEPS, 2)),
            DMA((STEPS, 2)),
            pltpu.SemaphoreType.REGULAR((2,)),
        ],
        compiler_params=pltpu.CompilerParams(
            collective_id=0, has_side_effects=True, vmem_limit_bytes=(36 if tail else 50) * 1024 * 1024),
    )(field_values, crowding)
    fields = [pltpu.with_memory_space_constraint(field, VMEM) for field in fields]
    out, done = pl.pallas_call(
        functools.partial(write_kernel, shape),
        out_shape=(jax.ShapeDtypeStruct(shape, dtype), VMEM((8, 128), dtype)),
        in_specs=[in_vmem],
        out_specs=(anywhere, in_vmem),
        scratch_shapes=[DMA((J,))],
        compiler_params=pltpu.CompilerParams(vmem_limit_bytes=1024 * 1024),
    )(fields[0])
    if not tail:
        return out
    piece = math.gcd(length, PIECE_ROWS)
    outer = VMEM((2, length, K, L), dtype)
    fresh = pl.pallas_call(
        functools.partial(tail_kernel, sizes, shape, length, piece),
        out_shape=outer,
        in_specs=[in_vmem] * 3,
        out_specs=in_vmem,
        scratch_shapes=[outer, DMA((2, length // piece)), DMA((2, length // piece))],
        compiler_params=pltpu.CompilerParams(
            collective_id=1, has_side_effects=True, vmem_limit_bytes=4 * 1024 * 1024),
    )(pltpu.with_memory_space_constraint(done, VMEM), *fields)
    return pl.pallas_call(
        functools.partial(patch_kernel, sizes, shape, length),
        out_shape=jax.ShapeDtypeStruct(shape, dtype),
        in_specs=[in_vmem, anywhere],
        out_specs=anywhere,
        scratch_shapes=[DMA((2,))],
        input_output_aliases={1: 0},
        compiler_params=pltpu.CompilerParams(vmem_limit_bytes=1024 * 1024),
    )(pltpu.with_memory_space_constraint(fresh, VMEM), out)


def solution(mesh):
    spec = P("lat", "lon", "lev", None)
    sizes = tuple(mesh.shape[axis] for axis in AXES)
    return jax.shard_map(
        functools.partial(local, sizes), mesh=mesh, in_specs=(spec, spec), out_specs=spec,
        check_vma=False,
    )
```

```python
import functools
import math

import jax
import jax.numpy as jnp
from jax import lax
from jax.experimental import pallas as pl
from jax.experimental.pallas import tpu as pltpu
from jax.sharding import PartitionSpec as P

STEPS = 3
CHUNK_ROWS = 4
WINDOW = 10
TAIL_CHUNKS = 3
PIECE_ROWS = 4
MESH = pl.DeviceIdType.MESH
AXES = ("lat", "lon", "lev")


def neighbours(sizes, axis):
    count, me = sizes[AXES.index(axis)], lax.axis_index(axis)
    return lax.rem(me + count - 1, count), lax.rem(me + 1, count)


def is_late(sizes):
    return lax.axis_index("lev") == sizes[AXES.index("lev")] - 1


def signal(sizes, axis, semaphore):
    for target in neighbours(sizes, axis):
        pl.semaphore_signal(semaphore, inc=1, device_id={axis: target}, device_id_type=MESH)


def enter(sizes, ready):
    barrier = pltpu.get_barrier_semaphore()
    odd = lax.rem(lax.axis_index("lat"), 2) == 1
    lead = lax.rem(lax.axis_index("lev"), 2) == 1
    odd_lon = lax.rem(lax.axis_index("lon"), 2) == 1
    follow = jnp.logical_not(lead)
    early = jnp.logical_and(follow, jnp.logical_not(odd_lon))
    answers = jnp.logical_and(follow, odd_lon)
    before, after = neighbours(sizes, "lat")

    def tell(semaphore, **target):
        pl.semaphore_signal(semaphore, inc=1, device_id=target, device_id_type=MESH)

    @pl.when(odd)
    def _():
        tell(barrier, lat=before)

    @pl.when(jnp.logical_not(odd))
    def _():
        tell(barrier, lat=after)
        tell(barrier, lat=before)

    pl.semaphore_wait(barrier, 1 + sum(
        n * flag.astype(jnp.int32) for n, flag in ((1, odd), (2, follow), (2, answers))))

    @pl.when(odd)
    def _():
        tell(ready.at[0], lat=after)

    def answer():
        pl.when(lead)(lambda: signal(sizes, "lev", barrier))
        pl.when(early)(lambda: signal(sizes, "lon", barrier))

        @pl.when(answers)
        def _():
            signal(sizes, "lon", ready.at[2])
            signal(sizes, "lev", ready.at[1])

    def await_lat():
        pl.when(jnp.logical_not(odd))(lambda: pl.semaphore_wait(ready.at[0], 1))

    def await_rest():
        @pl.when(early)
        def _():
            pl.semaphore_wait(ready.at[2], 2)
            signal(sizes, "lev", ready.at[1])

        pl.when(lead)(lambda: pl.semaphore_wait(ready.at[1], 2))

    return answer, await_lat, await_rest


def enter_together(sizes, axes):
    barrier = pltpu.get_barrier_semaphore()
    for axis in axes:
        signal(sizes, axis, barrier)
    pl.semaphore_wait(barrier, 2 * len(axes))


def march_kernel(sizes, shape, rows, tail, f_in, c_in, odd, even, crowd, jh, kh, kf,
                 load_sems, j_send, j_recv, i_send, i_recv, k_send, k_recv, ready):
    J, I, K, L = shape
    chunks = I // rows
    near = {axis: neighbours(sizes, axis) for axis in AXES}
    last_chunks = chunks - jnp.where(is_late(sizes), tail, 0) if tail else chunks

    fields = (even, odd)

    ahead = pltpu.make_async_copy(
        f_in.at[J - 1, pl.ds(0, rows)], even.at[J - 1, pl.ds(1, rows)], load_sems.at[2])
    even_lat = lax.rem(lax.axis_index("lat"), 2) == 0
    pl.when(even_lat)(ahead.start)

    if any(size % 2 for size in sizes):
        enter_together(sizes, AXES)
        answer = await_lat = await_rest = lambda: None
    else:
        answer, await_lat, await_rest = enter(sizes, ready)

    def remote(source, target, send, recv, axis, side):
        return pltpu.make_async_remote_copy(
            src_ref=source, dst_ref=target, send_sem=send, recv_sem=recv,
            device_id={axis: near[axis][side]}, device_id_type=MESH)

    def j_copy(step, side, chunk, loaded=False):
        j = (J - 1) * side
        if step == 0 and not loaded:
            source = f_in.at[j, pl.ds(chunk * rows, rows)]
        else:
            source = fields[step % 2].at[j, pl.ds(1 + chunk * rows, rows)]
        return remote(source, jh.at[step, 1 - side, pl.ds(chunk * rows, rows)],
                      j_send.at[step, side, chunk], j_recv.at[step, 1 - side, chunk], "lat", side)

    def i_copy(step, side):
        if step == 0:
            source = f_in.at[:, (I - 1) * side]
        else:
            source = fields[step % 2].at[:, 1 + (I - 1) * side]
        return remote(source, fields[step % 2].at[:, (I + 1) * (1 - side)],
                      i_send.at[step, side], i_recv.at[step, 1 - side], "lon", side)

    def k_copy(step, side):
        return remote(kf.at[step, side], kh.at[step, 1 - side],
                      k_send.at[step, side], k_recv.at[step, 1 - side], "lev", side)

    window = min(WINDOW, chunks - 1 - tail)

    @pl.when(even_lat)
    def _():
        ahead.wait()
        j_copy(0, 1, 0, loaded=True).start()

    pl.when(jnp.logical_not(even_lat))(lambda: j_copy(0, 1, 0).start())
    answer()
    await_lat()
    j_copy(0, 0, 0).start()

    @pl.loop(1, window)
    def _(chunk):
        for side in (0, 1):
            j_copy(0, side, chunk).start()

    load_inner = pltpu.make_async_copy(
        f_in.at[pl.ds(0, J - 1)], even.at[pl.ds(0, J - 1), pl.ds(1, I)], load_sems.at[0])
    load_outer = pltpu.make_async_copy(
        f_in.at[J - 1, pl.ds(rows, I - rows)], even.at[J - 1, pl.ds(1 + rows, I - rows)],
        load_sems.at[3])
    load_c = pltpu.make_async_copy(c_in, crowd, load_sems.at[1])
    pl.when(jnp.logical_not(even_lat))(ahead.start)
    load_inner.start()
    load_outer.start()
    load_c.start()
    await_rest()
    for side in (0, 1):
        i_copy(0, side).start()
    pl.when(jnp.logical_not(even_lat))(ahead.wait)
    load_inner.wait()
    load_outer.wait()

    @pl.loop(0, I)
    def _(i):
        for j in range(J):
            kf[0, 0, j, pl.ds(i, 1), :] = even[j, i + 1, 0:1, :]
            kf[0, 1, j, pl.ds(i, 1), :] = even[j, i + 1, K - 1:K, :]

    load_c.wait()
    for side in (0, 1):
        k_copy(0, side).start()

    at_k = lax.broadcasted_iota(jnp.int32, (K, L), 0)

    for step in range(STEPS):
        source, target = fields[step % 2], fields[(step + 1) % 2]
        last = step == STEPS - 1

        def update(i, j, below, above):
            middle = source[j, i + 1]
            total = source[j, i] + source[j, i + 2]
            if below is not None:
                total += below
            if above is not None:
                total += above
            total += jnp.where(at_k == 0, kh[step, 0, j, pl.ds(i, 1), :],
                               pltpu.roll(middle, 1, 0))
            total += jnp.where(at_k == K - 1, kh[step, 1, j, pl.ds(i, 1), :],
                               pltpu.roll(middle, K - 1, 0))
            return middle * (0.6 - 0.2 * (middle * crowd[j, i])) + 0.1 * total

        for side in (0, 1):
            i_copy(step, side).wait_recv()
            k_copy(step, side).wait_recv()
            if step >= 1:
                i_copy(step - 1, side).wait_send()

        if last:
            @pl.loop(window, last_chunks)
            def _(chunk):
                for side in (0, 1):
                    j_copy(step, side, chunk).start()

            @pl.loop(0, I)
            def _(i):
                for j in range(J):
                    target[j, i + 1] = update(
                        i, j, None if j == 0 else source[j - 1, i + 1],
                        None if j == J - 1 else source[j + 1, i + 1])

            @pl.loop(0, last_chunks)
            def _(chunk):
                for side in (0, 1):
                    j_copy(step, side, chunk).wait_recv()
                    j_copy(step, side, chunk).wait_send()

                @pl.loop(0, rows)
                def _(row):
                    i = chunk * rows + row
                    for side in (0, 1):
                        j = (J - 1) * side
                        target[j, i + 1] = target[j, i + 1] + 0.1 * jh[step, side, i]
        else:
            @pl.loop(0, chunks)
            def _(chunk):
                for side in (0, 1):
                    j_copy(step, side, chunk).wait_recv()
                    j_copy(step, side, chunk).wait_send()

                @pl.when(chunk + window < chunks)
                def _():
                    for side in (0, 1):
                        j_copy(step, side, chunk + window).start()

                @pl.when(chunk + window >= chunks)
                def _():
                    for side in (0, 1):
                        j_copy(step + 1, side, chunk + window - chunks).start()

                @pl.loop(0, rows)
                def _(row):
                    i = chunk * rows + row
                    for j in range(J):
                        new = update(
                            i, j, jh[step, 0, i] if j == 0 else source[j - 1, i + 1],
                            jh[step, 1, i] if j == J - 1 else source[j + 1, i + 1])
                        target[j, i + 1] = new
                        kf[step + 1, 0, j, pl.ds(i, 1), :] = new[0:1]
                        kf[step + 1, 1, j, pl.ds(i, 1), :] = new[K - 1:K]

            for side in (0, 1):
                i_copy(step + 1, side).start()
                k_copy(step + 1, side).start()

    for side in (0, 1):
        i_copy(STEPS - 1, side).wait_send()
        for step in range(STEPS):
            k_copy(step, side).wait_send()


def write_kernel(shape, held, out, done, sems):
    J, I = shape[:2]
    copies = [pltpu.make_async_copy(held.at[j, pl.ds(1, I)], out.at[j], sems.at[j])
              for j in range(J)]
    for copy in copies:
        copy.start()
    done[...] = jnp.zeros_like(done)
    for copy in copies:
        copy.wait()


def tail_kernel(sizes, shape, length, rows, done, held, even, fresh, halo, sends, recvs):
    J, I = shape[:2]
    first = I - length

    @pl.when(is_late(sizes))
    def _():
        enter_together(sizes, ("lat",))
        near = neighbours(sizes, "lat")

        def j_copy(side, piece):
            return pltpu.make_async_remote_copy(
                src_ref=even.at[(J - 1) * side, pl.ds(1 + first + piece * rows, rows)],
                dst_ref=halo.at[1 - side, pl.ds(piece * rows, rows)],
                send_sem=sends.at[side, piece], recv_sem=recvs.at[1 - side, piece],
                device_id={"lat": near[side]}, device_id_type=MESH)

        odd = lax.rem(lax.axis_index("lat"), 2) == 1

        @pl.loop(0, length // rows)
        def _(piece):
            pl.when(odd)(lambda: j_copy(1, piece).start())
            j_copy(0, piece).start()
            pl.when(jnp.logical_not(odd))(lambda: j_copy(1, piece).start())

        @pl.loop(0, length // rows)
        def _(piece):
            for side in (0, 1):
                j_copy(side, piece).wait_recv()

            @pl.loop(0, rows)
            def _(row):
                i = piece * rows + row
                for side in (0, 1):
                    fresh[side, i] = held[(J - 1) * side, 1 + first + i] + 0.1 * halo[side, i]

        @pl.loop(0, length // rows)
        def _(piece):
            for side in (0, 1):
                j_copy(side, piece).wait_send()


def patch_kernel(sizes, shape, length, fresh, before, out, sems):
    J, I = shape[:2]

    @pl.when(is_late(sizes))
    def _():
        copies = [
            pltpu.make_async_copy(
                fresh.at[side], out.at[(J - 1) * side, pl.ds(I - length, length)], sems.at[side])
            for side in (0, 1)]
        for copy in copies:
            copy.start()
        for copy in copies:
            copy.wait()


def local(sizes, field_values, crowding):
    J, I, K, L = shape = field_values.shape
    rows = math.gcd(I, CHUNK_ROWS)
    chunks = I // rows
    tail = TAIL_CHUNKS if J >= 2 and chunks > TAIL_CHUNKS + 1 else 0
    length = tail * rows
    dtype = field_values.dtype
    DMA = pltpu.SemaphoreType.DMA
    VMEM = pltpu.VMEM
    whole = VMEM((J, I + 2, K, L), dtype)
    in_vmem, anywhere = pl.BlockSpec(memory_space=VMEM), pl.BlockSpec(memory_space=pl.ANY)
    fields = pl.pallas_call(
        functools.partial(march_kernel, sizes, shape, rows, tail),
        out_shape=(whole,) * (2 if tail else 1),
        in_specs=[anywhere] * 2,
        out_specs=(in_vmem,) * (2 if tail else 1),
        scratch_shapes=[whole] * (0 if tail else 1) + [
            VMEM(shape, dtype),
            VMEM((STEPS, 2, I, K, L), dtype),
            VMEM((STEPS, 2, J, I, L), dtype),
            VMEM((STEPS, 2, J, I, L), dtype),
            DMA((4,)),
            DMA((STEPS, 2, chunks)),
            DMA((STEPS, 2, chunks)),
            DMA((STEPS, 2)),
            DMA((STEPS, 2)),
            DMA((STEPS, 2)),
            DMA((STEPS, 2)),
            pltpu.SemaphoreType.REGULAR((3,)),
        ],
        compiler_params=pltpu.CompilerParams(
            collective_id=0, has_side_effects=True, vmem_limit_bytes=(36 if tail else 50) * 1024 * 1024),
    )(field_values, crowding)
    fields = [pltpu.with_memory_space_constraint(field, VMEM) for field in fields]
    out, done = pl.pallas_call(
        functools.partial(write_kernel, shape),
        out_shape=(jax.ShapeDtypeStruct(shape, dtype), VMEM((8, 128), dtype)),
        in_specs=[in_vmem],
        out_specs=(anywhere, in_vmem),
        scratch_shapes=[DMA((J,))],
        compiler_params=pltpu.CompilerParams(vmem_limit_bytes=1024 * 1024),
    )(fields[0])
    if not tail:
        return out
    piece = math.gcd(length, PIECE_ROWS)
    outer = VMEM((2, length, K, L), dtype)
    fresh = pl.pallas_call(
        functools.partial(tail_kernel, sizes, shape, length, piece),
        out_shape=outer,
        in_specs=[in_vmem] * 3,
        out_specs=in_vmem,
        scratch_shapes=[outer, DMA((2, length // piece)), DMA((2, length // piece))],
        compiler_params=pltpu.CompilerParams(
            collective_id=1, has_side_effects=True, vmem_limit_bytes=4 * 1024 * 1024),
    )(pltpu.with_memory_space_constraint(done, VMEM), *fields)
    return pl.pallas_call(
        functools.partial(patch_kernel, sizes, shape, length),
        out_shape=jax.ShapeDtypeStruct(shape, dtype),
        in_specs=[in_vmem, anywhere],
        out_specs=anywhere,
        scratch_shapes=[DMA((2,))],
        input_output_aliases={1: 0},
        compiler_params=pltpu.CompilerParams(vmem_limit_bytes=1024 * 1024),
    )(pltpu.with_memory_space_constraint(fresh, VMEM), out)


def solution(mesh):
    spec = P("lat", "lon", "lev", None)
    sizes = tuple(mesh.shape[axis] for axis in AXES)
    return jax.shard_map(
        functools.partial(local, sizes), mesh=mesh, in_specs=(spec, spec), out_specs=spec,
        check_vma=False,
    )
```

```python
import functools
import math

import jax
import jax.numpy as jnp
from jax import lax
from jax.experimental import pallas as pl
from jax.experimental.pallas import tpu as pltpu
from jax.sharding import PartitionSpec as P

STEPS = 3
CHUNK_ROWS = 4
WINDOW = 10
TAIL_CHUNKS = 3
PIECE_ROWS = 4
MESH = pl.DeviceIdType.MESH
AXES = ("lat", "lon", "lev")


def neighbours(sizes, axis):
    count, me = sizes[AXES.index(axis)], lax.axis_index(axis)
    return lax.rem(me + count - 1, count), lax.rem(me + 1, count)


def is_late(sizes):
    return lax.axis_index("lev") == sizes[AXES.index("lev")] - 1


def signal(sizes, axis, semaphore):
    for target in neighbours(sizes, axis):
        pl.semaphore_signal(semaphore, inc=1, device_id={axis: target}, device_id_type=MESH)


def enter(sizes, ready):
    barrier = pltpu.get_barrier_semaphore()
    odd = lax.rem(lax.axis_index("lat"), 2) == 1
    lead = lax.rem(lax.axis_index("lev"), 2) == 1
    odd_lon = lax.rem(lax.axis_index("lon"), 2) == 1
    follow = jnp.logical_not(lead)
    early = jnp.logical_and(follow, jnp.logical_not(odd_lon))
    answers = jnp.logical_and(follow, odd_lon)
    before, after = neighbours(sizes, "lat")

    def tell(semaphore, **target):
        pl.semaphore_signal(semaphore, inc=1, device_id=target, device_id_type=MESH)

    @pl.when(odd)
    def _():
        tell(barrier, lat=before)

    @pl.when(jnp.logical_not(odd))
    def _():
        tell(barrier, lat=after)
        tell(barrier, lat=before)

    pl.semaphore_wait(barrier, 1 + sum(
        n * flag.astype(jnp.int32) for n, flag in ((1, odd), (2, follow), (2, answers))))

    @pl.when(odd)
    def _():
        tell(ready.at[0], lat=after)

    def answer():
        pl.when(lead)(lambda: signal(sizes, "lev", barrier))
        pl.when(early)(lambda: signal(sizes, "lon", barrier))

        @pl.when(answers)
        def _():
            signal(sizes, "lon", ready.at[2])
            signal(sizes, "lev", ready.at[1])

    def await_lat():
        pl.when(jnp.logical_not(odd))(lambda: pl.semaphore_wait(ready.at[0], 1))

    def await_rest():
        @pl.when(early)
        def _():
            pl.semaphore_wait(ready.at[2], 2)
            signal(sizes, "lev", ready.at[1])

        pl.when(lead)(lambda: pl.semaphore_wait(ready.at[1], 2))

    return answer, await_lat, await_rest


def enter_together(sizes, axes):
    barrier = pltpu.get_barrier_semaphore()
    for axis in axes:
        signal(sizes, axis, barrier)
    pl.semaphore_wait(barrier, 2 * len(axes))


def march_kernel(sizes, shape, rows, tail, f_in, c_in, odd, even, crowd, jh, kh, kf,
                 load_sems, j_send, j_recv, i_send, i_recv, k_send, k_recv, ready):
    J, I, K, L = shape
    chunks = I // rows
    near = {axis: neighbours(sizes, axis) for axis in AXES}
    last_chunks = chunks - jnp.where(is_late(sizes), tail, 0) if tail else chunks

    fields = (even, odd)

    ahead = pltpu.make_async_copy(
        f_in.at[J - 1, pl.ds(0, rows)], even.at[J - 1, pl.ds(1, rows)], load_sems.at[2])
    even_lat = lax.rem(lax.axis_index("lat"), 2) == 0
    pl.when(even_lat)(ahead.start)

    if any(size % 2 for size in sizes):
        enter_together(sizes, AXES)
        answer = await_lat = await_rest = lambda: None
    else:
        answer, await_lat, await_rest = enter(sizes, ready)

    def remote(source, target, send, recv, axis, side):
        return pltpu.make_async_remote_copy(
            src_ref=source, dst_ref=target, send_sem=send, recv_sem=recv,
            device_id={axis: near[axis][side]}, device_id_type=MESH)

    def j_copy(step, side, chunk, loaded=False):
        j = (J - 1) * side
        if step == 0 and not loaded:
            source = f_in.at[j, pl.ds(chunk * rows, rows)]
        else:
            source = fields[step % 2].at[j, pl.ds(1 + chunk * rows, rows)]
        return remote(source, jh.at[step, 1 - side, pl.ds(chunk * rows, rows)],
                      j_send.at[step, side, chunk], j_recv.at[step, 1 - side, chunk], "lat", side)

    def i_copy(step, side):
        if step == 0:
            source = f_in.at[:, (I - 1) * side]
        else:
            source = fields[step % 2].at[:, 1 + (I - 1) * side]
        return remote(source, fields[step % 2].at[:, (I + 1) * (1 - side)],
                      i_send.at[step, side], i_recv.at[step, 1 - side], "lon", side)

    def k_copy(step, side):
        return remote(kf.at[step, side], kh.at[step, 1 - side],
                      k_send.at[step, side], k_recv.at[step, 1 - side], "lev", side)

    window = min(WINDOW, chunks - 1 - tail)

    @pl.when(even_lat)
    def _():
        ahead.wait()
        j_copy(0, 1, 0, loaded=True).start()

    pl.when(jnp.logical_not(even_lat))(lambda: j_copy(0, 1, 0).start())
    answer()
    await_lat()
    j_copy(0, 0, 0).start()

    @pl.loop(1, window)
    def _(chunk):
        for side in (0, 1):
            j_copy(0, side, chunk).start()

    load_inner = pltpu.make_async_copy(
        f_in.at[pl.ds(0, J - 1)], even.at[pl.ds(0, J - 1), pl.ds(1, I)], load_sems.at[0])
    load_outer = pltpu.make_async_copy(
        f_in.at[J - 1, pl.ds(rows, I - rows)], even.at[J - 1, pl.ds(1 + rows, I - rows)],
        load_sems.at[3])
    load_c = pltpu.make_async_copy(c_in, crowd, load_sems.at[1])
    pl.when(jnp.logical_not(even_lat))(ahead.start)
    load_inner.start()
    load_outer.start()
    load_c.start()
    await_rest()
    for side in (0, 1):
        i_copy(0, side).start()
    pl.when(jnp.logical_not(even_lat))(ahead.wait)
    load_inner.wait()
    load_outer.wait()

    @pl.loop(0, I)
    def _(i):
        for j in range(J):
            kf[0, 0, j, pl.ds(i, 1), :] = even[j, i + 1, 0:1, :]
            kf[0, 1, j, pl.ds(i, 1), :] = even[j, i + 1, K - 1:K, :]

    load_c.wait()
    for side in (0, 1):
        k_copy(0, side).start()

    at_k = lax.broadcasted_iota(jnp.int32, (K, L), 0)

    for step in range(STEPS):
        source, target = fields[step % 2], fields[(step + 1) % 2]
        last = step == STEPS - 1

        def update(i, j, below, above):
            middle = source[j, i + 1]
            total = source[j, i] + source[j, i + 2]
            if below is not None:
                total += below
            if above is not None:
                total += above
            total += jnp.where(at_k == 0, kh[step, 0, j, pl.ds(i, 1), :],
                               pltpu.roll(middle, 1, 0))
            total += jnp.where(at_k == K - 1, kh[step, 1, j, pl.ds(i, 1), :],
                               pltpu.roll(middle, K - 1, 0))
            return middle * (0.6 - 0.2 * (middle * crowd[j, i])) + 0.1 * total

        for side in (0, 1):
            i_copy(step, side).wait_recv()
            k_copy(step, side).wait_recv()
            if step >= 1:
                i_copy(step - 1, side).wait_send()

        if last:
            @pl.loop(window, last_chunks)
            def _(chunk):
                for side in (0, 1):
                    j_copy(step, side, chunk).start()

            @pl.loop(0, I)
            def _(i):
                for j in range(J):
                    target[j, i + 1] = update(
                        i, j, None if j == 0 else source[j - 1, i + 1],
                        None if j == J - 1 else source[j + 1, i + 1])

            @pl.loop(0, last_chunks)
            def _(chunk):
                for side in (0, 1):
                    j_copy(step, side, chunk).wait_recv()
                    j_copy(step, side, chunk).wait_send()

                @pl.loop(0, rows)
                def _(row):
                    i = chunk * rows + row
                    for side in (0, 1):
                        j = (J - 1) * side
                        target[j, i + 1] = target[j, i + 1] + 0.1 * jh[step, side, i]
        else:
            @pl.loop(0, chunks)
            def _(chunk):
                for side in (0, 1):
                    j_copy(step, side, chunk).wait_recv()
                    j_copy(step, side, chunk).wait_send()

                @pl.when(chunk + window < chunks)
                def _():
                    for side in (0, 1):
                        j_copy(step, side, chunk + window).start()

                @pl.when(chunk + window >= chunks)
                def _():
                    for side in (0, 1):
                        j_copy(step + 1, side, chunk + window - chunks).start()

                @pl.loop(0, rows)
                def _(row):
                    i = chunk * rows + row
                    for j in range(J):
                        new = update(
                            i, j, jh[step, 0, i] if j == 0 else source[j - 1, i + 1],
                            jh[step, 1, i] if j == J - 1 else source[j + 1, i + 1])
                        target[j, i + 1] = new
                        kf[step + 1, 0, j, pl.ds(i, 1), :] = new[0:1]
                        kf[step + 1, 1, j, pl.ds(i, 1), :] = new[K - 1:K]

            for side in (0, 1):
                i_copy(step + 1, side).start()
                k_copy(step + 1, side).start()

    for side in (0, 1):
        i_copy(STEPS - 1, side).wait_send()
        for step in range(STEPS):
            k_copy(step, side).wait_send()


def write_kernel(shape, held, out, done, sems):
    J, I = shape[:2]
    copies = [pltpu.make_async_copy(held.at[j, pl.ds(1, I)], out.at[j], sems.at[j])
              for j in range(J)]
    for copy in copies:
        copy.start()
    done[...] = jnp.zeros_like(done)
    for copy in copies:
        copy.wait()


def tail_kernel(sizes, shape, length, rows, done, held, even, fresh, halo, sends, recvs):
    J, I = shape[:2]
    first = I - length

    @pl.when(is_late(sizes))
    def _():
        enter_together(sizes, ("lat",))
        near = neighbours(sizes, "lat")

        def j_copy(side, piece):
            return pltpu.make_async_remote_copy(
                src_ref=even.at[(J - 1) * side, pl.ds(1 + first + piece * rows, rows)],
                dst_ref=halo.at[1 - side, pl.ds(piece * rows, rows)],
                send_sem=sends.at[side, piece], recv_sem=recvs.at[1 - side, piece],
                device_id={"lat": near[side]}, device_id_type=MESH)

        odd = lax.rem(lax.axis_index("lat"), 2) == 1

        @pl.loop(0, length // rows)
        def _(piece):
            pl.when(odd)(lambda: j_copy(1, piece).start())
            j_copy(0, piece).start()
            pl.when(jnp.logical_not(odd))(lambda: j_copy(1, piece).start())

        @pl.loop(0, length // rows)
        def _(piece):
            for side in (0, 1):
                j_copy(side, piece).wait_recv()

            @pl.loop(0, rows)
            def _(row):
                i = piece * rows + row
                for side in (0, 1):
                    fresh[side, i] = held[(J - 1) * side, 1 + first + i] + 0.1 * halo[side, i]

        @pl.loop(0, length // rows)
        def _(piece):
            for side in (0, 1):
                j_copy(side, piece).wait_send()


def patch_kernel(sizes, shape, length, rows, fresh, before, out, sems):
    J, I = shape[:2]

    @pl.when(is_late(sizes))
    def _():
        copies = [
            pltpu.make_async_copy(
                fresh.at[side, pl.ds(part * rows, rows)],
                out.at[(J - 1) * side, pl.ds(I - length + part * rows, rows)],
                sems.at[side, part])
            for part in range(length // rows) for side in (0, 1)]
        for copy in copies:
            copy.start()
        for copy in copies:
            copy.wait()


def local(sizes, field_values, crowding):
    J, I, K, L = shape = field_values.shape
    rows = math.gcd(I, CHUNK_ROWS)
    chunks = I // rows
    tail = TAIL_CHUNKS if J >= 2 and chunks > TAIL_CHUNKS + 1 else 0
    length = tail * rows
    dtype = field_values.dtype
    DMA = pltpu.SemaphoreType.DMA
    VMEM = pltpu.VMEM
    whole = VMEM((J, I + 2, K, L), dtype)
    in_vmem, anywhere = pl.BlockSpec(memory_space=VMEM), pl.BlockSpec(memory_space=pl.ANY)
    fields = pl.pallas_call(
        functools.partial(march_kernel, sizes, shape, rows, tail),
        out_shape=(whole,) * (2 if tail else 1),
        in_specs=[anywhere] * 2,
        out_specs=(in_vmem,) * (2 if tail else 1),
        scratch_shapes=[whole] * (0 if tail else 1) + [
            VMEM(shape, dtype),
            VMEM((STEPS, 2, I, K, L), dtype),
            VMEM((STEPS, 2, J, I, L), dtype),
            VMEM((STEPS, 2, J, I, L), dtype),
            DMA((4,)),
            DMA((STEPS, 2, chunks)),
            DMA((STEPS, 2, chunks)),
            DMA((STEPS, 2)),
            DMA((STEPS, 2)),
            DMA((STEPS, 2)),
            DMA((STEPS, 2)),
            pltpu.SemaphoreType.REGULAR((3,)),
        ],
        compiler_params=pltpu.CompilerParams(
            collective_id=0, has_side_effects=True, vmem_limit_bytes=(36 if tail else 50) * 1024 * 1024),
    )(field_values, crowding)
    fields = [pltpu.with_memory_space_constraint(field, VMEM) for field in fields]
    out, done = pl.pallas_call(
        functools.partial(write_kernel, shape),
        out_shape=(jax.ShapeDtypeStruct(shape, dtype), VMEM((8, 128), dtype)),
        in_specs=[in_vmem],
        out_specs=(anywhere, in_vmem),
        scratch_shapes=[DMA((J,))],
        compiler_params=pltpu.CompilerParams(vmem_limit_bytes=1024 * 1024),
    )(fields[0])
    if not tail:
        return out
    piece = math.gcd(length, PIECE_ROWS)
    outer = VMEM((2, length, K, L), dtype)
    fresh = pl.pallas_call(
        functools.partial(tail_kernel, sizes, shape, length, piece),
        out_shape=outer,
        in_specs=[in_vmem] * 3,
        out_specs=in_vmem,
        scratch_shapes=[outer, DMA((2, length // piece)), DMA((2, length // piece))],
        compiler_params=pltpu.CompilerParams(
            collective_id=1, has_side_effects=True, vmem_limit_bytes=4 * 1024 * 1024),
    )(pltpu.with_memory_space_constraint(done, VMEM), *fields)
    return pl.pallas_call(
        functools.partial(patch_kernel, sizes, shape, length, piece),
        out_shape=jax.ShapeDtypeStruct(shape, dtype),
        in_specs=[in_vmem, anywhere],
        out_specs=anywhere,
        scratch_shapes=[DMA((2, length // piece))],
        input_output_aliases={1: 0},
        compiler_params=pltpu.CompilerParams(vmem_limit_bytes=1024 * 1024),
    )(pltpu.with_memory_space_constraint(fresh, VMEM), out)


def solution(mesh):
    spec = P("lat", "lon", "lev", None)
    sizes = tuple(mesh.shape[axis] for axis in AXES)
    return jax.shard_map(
        functools.partial(local, sizes), mesh=mesh, in_specs=(spec, spec), out_specs=spec,
        check_vma=False,
    )
```

```python
import functools
import math

import jax
import jax.numpy as jnp
from jax import lax
from jax.experimental import pallas as pl
from jax.experimental.pallas import tpu as pltpu
from jax.sharding import PartitionSpec as P

STEPS = 3
CHUNK_ROWS = 4
WINDOW = 10
TAIL_CHUNKS = 3
PIECE_ROWS = 4
MESH = pl.DeviceIdType.MESH
AXES = ("lat", "lon", "lev")


def neighbours(sizes, axis):
    count, me = sizes[AXES.index(axis)], lax.axis_index(axis)
    return lax.rem(me + count - 1, count), lax.rem(me + 1, count)


def is_late(sizes):
    return lax.axis_index("lev") == sizes[AXES.index("lev")] - 1


def signal(sizes, axis, semaphore):
    for target in neighbours(sizes, axis):
        pl.semaphore_signal(semaphore, inc=1, device_id={axis: target}, device_id_type=MESH)


def enter(sizes, ready):
    barrier = pltpu.get_barrier_semaphore()
    odd = lax.rem(lax.axis_index("lat"), 2) == 1
    lead = lax.rem(lax.axis_index("lev"), 2) == 1
    odd_lon = lax.rem(lax.axis_index("lon"), 2) == 1
    follow = jnp.logical_not(lead)
    early = jnp.logical_and(follow, jnp.logical_not(odd_lon))
    answers = jnp.logical_and(follow, odd_lon)
    before, after = neighbours(sizes, "lat")

    def tell(semaphore, **target):
        pl.semaphore_signal(semaphore, inc=1, device_id=target, device_id_type=MESH)

    @pl.when(odd)
    def _():
        tell(barrier, lat=before)

    @pl.when(jnp.logical_not(odd))
    def _():
        tell(barrier, lat=after)
        tell(barrier, lat=before)

    pl.semaphore_wait(barrier, 1 + sum(
        n * flag.astype(jnp.int32) for n, flag in ((1, odd), (2, follow), (2, answers))))

    @pl.when(odd)
    def _():
        tell(ready.at[0], lat=after)

    def answer():
        pl.when(lead)(lambda: signal(sizes, "lev", barrier))
        pl.when(early)(lambda: signal(sizes, "lon", barrier))

        @pl.when(answers)
        def _():
            signal(sizes, "lon", ready.at[2])
            signal(sizes, "lev", ready.at[1])

    def await_lat():
        pl.when(jnp.logical_not(odd))(lambda: pl.semaphore_wait(ready.at[0], 1))

    def await_rest():
        @pl.when(early)
        def _():
            pl.semaphore_wait(ready.at[2], 2)
            signal(sizes, "lev", ready.at[1])

        pl.when(lead)(lambda: pl.semaphore_wait(ready.at[1], 2))

    return answer, await_lat, await_rest


def enter_together(sizes, axes):
    barrier = pltpu.get_barrier_semaphore()
    for axis in axes:
        signal(sizes, axis, barrier)
    pl.semaphore_wait(barrier, 2 * len(axes))


def march_kernel(sizes, shape, rows, tail, f_in, c_in, odd, even, crowd, jh, kh, kf,
                 load_sems, j_send, j_recv, i_send, i_recv, k_send, k_recv, ready):
    J, I, K, L = shape
    chunks = I // rows
    near = {axis: neighbours(sizes, axis) for axis in AXES}
    last_chunks = chunks - jnp.where(is_late(sizes), tail, 0) if tail else chunks

    fields = (even, odd)

    ahead = pltpu.make_async_copy(
        f_in.at[J - 1, pl.ds(0, rows)], even.at[J - 1, pl.ds(1, rows)], load_sems.at[2])
    even_lat = lax.rem(lax.axis_index("lat"), 2) == 0
    pl.when(even_lat)(ahead.start)

    if any(size % 2 for size in sizes):
        enter_together(sizes, AXES)
        answer = await_lat = await_rest = lambda: None
    else:
        answer, await_lat, await_rest = enter(sizes, ready)

    def remote(source, target, send, recv, axis, side):
        return pltpu.make_async_remote_copy(
            src_ref=source, dst_ref=target, send_sem=send, recv_sem=recv,
            device_id={axis: near[axis][side]}, device_id_type=MESH)

    def j_copy(step, side, chunk, loaded=False):
        j = (J - 1) * side
        if step == 0 and not loaded:
            source = f_in.at[j, pl.ds(chunk * rows, rows)]
        else:
            source = fields[step % 2].at[j, pl.ds(1 + chunk * rows, rows)]
        return remote(source, jh.at[step, 1 - side, pl.ds(chunk * rows, rows)],
                      j_send.at[step, side, chunk], j_recv.at[step, 1 - side, chunk], "lat", side)

    def i_copy(step, side):
        if step == 0:
            source = f_in.at[:, (I - 1) * side]
        else:
            source = fields[step % 2].at[:, 1 + (I - 1) * side]
        return remote(source, fields[step % 2].at[:, (I + 1) * (1 - side)],
                      i_send.at[step, side], i_recv.at[step, 1 - side], "lon", side)

    def k_copy(step, side):
        return remote(kf.at[step, side], kh.at[step, 1 - side],
                      k_send.at[step, side], k_recv.at[step, 1 - side], "lev", side)

    window = min(WINDOW, chunks - 1 - tail)

    @pl.when(even_lat)
    def _():
        ahead.wait()
        j_copy(0, 1, 0, loaded=True).start()

    pl.when(jnp.logical_not(even_lat))(lambda: j_copy(0, 1, 0).start())
    answer()
    await_lat()
    j_copy(0, 0, 0).start()

    @pl.loop(1, window)
    def _(chunk):
        for side in (0, 1):
            j_copy(0, side, chunk).start()

    load_inner = pltpu.make_async_copy(
        f_in.at[pl.ds(0, J - 1)], even.at[pl.ds(0, J - 1), pl.ds(1, I)], load_sems.at[0])
    load_outer = pltpu.make_async_copy(
        f_in.at[J - 1, pl.ds(rows, I - rows)], even.at[J - 1, pl.ds(1 + rows, I - rows)],
        load_sems.at[3])
    load_c = pltpu.make_async_copy(c_in, crowd, load_sems.at[1])
    pl.when(jnp.logical_not(even_lat))(ahead.start)
    load_inner.start()
    load_outer.start()
    load_c.start()
    await_rest()
    for side in (0, 1):
        i_copy(0, side).start()
    pl.when(jnp.logical_not(even_lat))(ahead.wait)
    load_inner.wait()
    load_outer.wait()

    @pl.loop(0, I)
    def _(i):
        for j in range(J):
            kf[0, 0, j, pl.ds(i, 1), :] = even[j, i + 1, 0:1, :]
            kf[0, 1, j, pl.ds(i, 1), :] = even[j, i + 1, K - 1:K, :]

    load_c.wait()
    for side in (0, 1):
        k_copy(0, side).start()

    at_k = lax.broadcasted_iota(jnp.int32, (K, L), 0)

    for step in range(STEPS):
        source, target = fields[step % 2], fields[(step + 1) % 2]
        last = step == STEPS - 1

        def update(i, j, below, above):
            middle = source[j, i + 1]
            total = source[j, i] + source[j, i + 2]
            if below is not None:
                total += below
            if above is not None:
                total += above
            total += jnp.where(at_k == 0, kh[step, 0, j, pl.ds(i, 1), :],
                               pltpu.roll(middle, 1, 0))
            total += jnp.where(at_k == K - 1, kh[step, 1, j, pl.ds(i, 1), :],
                               pltpu.roll(middle, K - 1, 0))
            return middle * (0.6 - 0.2 * (middle * crowd[j, i])) + 0.1 * total

        for side in (0, 1):
            i_copy(step, side).wait_recv()
            k_copy(step, side).wait_recv()
            if step >= 1:
                i_copy(step - 1, side).wait_send()

        if last:
            @pl.loop(window, last_chunks)
            def _(chunk):
                for side in (0, 1):
                    j_copy(step, side, chunk).start()

            @pl.loop(0, I)
            def _(i):
                for j in range(J):
                    target[j, i + 1] = update(
                        i, j, None if j == 0 else source[j - 1, i + 1],
                        None if j == J - 1 else source[j + 1, i + 1])

            @pl.loop(0, last_chunks)
            def _(chunk):
                for side in (0, 1):
                    j_copy(step, side, chunk).wait_recv()
                    j_copy(step, side, chunk).wait_send()

                @pl.loop(0, rows)
                def _(row):
                    i = chunk * rows + row
                    for side in (0, 1):
                        j = (J - 1) * side
                        target[j, i + 1] = target[j, i + 1] + 0.1 * jh[step, side, i]
        else:
            @pl.loop(0, chunks)
            def _(chunk):
                for side in (0, 1):
                    j_copy(step, side, chunk).wait_recv()
                    j_copy(step, side, chunk).wait_send()

                @pl.when(chunk + window < chunks)
                def _():
                    for side in (0, 1):
                        j_copy(step, side, chunk + window).start()

                @pl.when(chunk + window >= chunks)
                def _():
                    for side in (0, 1):
                        j_copy(step + 1, side, chunk + window - chunks).start()

                @pl.loop(0, rows)
                def _(row):
                    i = chunk * rows + row
                    for j in range(J):
                        new = update(
                            i, j, jh[step, 0, i] if j == 0 else source[j - 1, i + 1],
                            jh[step, 1, i] if j == J - 1 else source[j + 1, i + 1])
                        target[j, i + 1] = new
                        kf[step + 1, 0, j, pl.ds(i, 1), :] = new[0:1]
                        kf[step + 1, 1, j, pl.ds(i, 1), :] = new[K - 1:K]

            for side in (0, 1):
                i_copy(step + 1, side).start()
                k_copy(step + 1, side).start()

    for side in (0, 1):
        i_copy(STEPS - 1, side).wait_send()
        for step in range(STEPS):
            k_copy(step, side).wait_send()


def write_kernel(sizes, shape, length, held, out, done, sems):
    J, I = shape[:2]

    def write(tail):
        copies = []
        for j in range(J):
            count = I - tail if j in (0, J - 1) else I
            copies.append(pltpu.make_async_copy(
                held.at[j, pl.ds(1, count)], out.at[j, pl.ds(0, count)], sems.at[j]))
        for copy in copies:
            copy.start()
        for copy in copies:
            copy.wait()

    done[...] = jnp.zeros_like(done)
    late = is_late(sizes)
    pl.when(late)(lambda: write(length))
    pl.when(jnp.logical_not(late))(lambda: write(0))


def tail_kernel(sizes, shape, length, rows, done, held, even, fresh, halo, sends, recvs):
    J, I = shape[:2]
    first = I - length

    @pl.when(is_late(sizes))
    def _():
        enter_together(sizes, ("lat",))
        near = neighbours(sizes, "lat")

        def j_copy(side, piece):
            return pltpu.make_async_remote_copy(
                src_ref=even.at[(J - 1) * side, pl.ds(1 + first + piece * rows, rows)],
                dst_ref=halo.at[1 - side, pl.ds(piece * rows, rows)],
                send_sem=sends.at[side, piece], recv_sem=recvs.at[1 - side, piece],
                device_id={"lat": near[side]}, device_id_type=MESH)

        odd = lax.rem(lax.axis_index("lat"), 2) == 1

        @pl.loop(0, length // rows)
        def _(piece):
            pl.when(odd)(lambda: j_copy(1, piece).start())
            j_copy(0, piece).start()
            pl.when(jnp.logical_not(odd))(lambda: j_copy(1, piece).start())

        @pl.loop(0, length // rows)
        def _(piece):
            for side in (0, 1):
                j_copy(side, piece).wait_recv()

            @pl.loop(0, rows)
            def _(row):
                i = piece * rows + row
                for side in (0, 1):
                    fresh[side, i] = held[(J - 1) * side, 1 + first + i] + 0.1 * halo[side, i]

        @pl.loop(0, length // rows)
        def _(piece):
            for side in (0, 1):
                j_copy(side, piece).wait_send()


def patch_kernel(sizes, shape, length, rows, fresh, before, out, sems):
    J, I = shape[:2]

    @pl.when(is_late(sizes))
    def _():
        copies = [
            pltpu.make_async_copy(
                fresh.at[side, pl.ds(part * rows, rows)],
                out.at[(J - 1) * side, pl.ds(I - length + part * rows, rows)],
                sems.at[side, part])
            for part in range(length // rows) for side in (0, 1)]
        for copy in copies:
            copy.start()
        for copy in copies:
            copy.wait()


def local(sizes, field_values, crowding):
    J, I, K, L = shape = field_values.shape
    rows = math.gcd(I, CHUNK_ROWS)
    chunks = I // rows
    tail = TAIL_CHUNKS if J >= 2 and chunks > TAIL_CHUNKS + 1 else 0
    length = tail * rows
    dtype = field_values.dtype
    DMA = pltpu.SemaphoreType.DMA
    VMEM = pltpu.VMEM
    whole = VMEM((J, I + 2, K, L), dtype)
    in_vmem, anywhere = pl.BlockSpec(memory_space=VMEM), pl.BlockSpec(memory_space=pl.ANY)
    fields = pl.pallas_call(
        functools.partial(march_kernel, sizes, shape, rows, tail),
        out_shape=(whole,) * (2 if tail else 1),
        in_specs=[anywhere] * 2,
        out_specs=(in_vmem,) * (2 if tail else 1),
        scratch_shapes=[whole] * (0 if tail else 1) + [
            VMEM(shape, dtype),
            VMEM((STEPS, 2, I, K, L), dtype),
            VMEM((STEPS, 2, J, I, L), dtype),
            VMEM((STEPS, 2, J, I, L), dtype),
            DMA((4,)),
            DMA((STEPS, 2, chunks)),
            DMA((STEPS, 2, chunks)),
            DMA((STEPS, 2)),
            DMA((STEPS, 2)),
            DMA((STEPS, 2)),
            DMA((STEPS, 2)),
            pltpu.SemaphoreType.REGULAR((3,)),
        ],
        compiler_params=pltpu.CompilerParams(
            collective_id=0, has_side_effects=True, vmem_limit_bytes=(36 if tail else 50) * 1024 * 1024),
    )(field_values, crowding)
    fields = [pltpu.with_memory_space_constraint(field, VMEM) for field in fields]
    out, done = pl.pallas_call(
        functools.partial(write_kernel, sizes, shape, length),
        out_shape=(jax.ShapeDtypeStruct(shape, dtype), VMEM((8, 128), dtype)),
        in_specs=[in_vmem],
        out_specs=(anywhere, in_vmem),
        scratch_shapes=[DMA((J,))],
        compiler_params=pltpu.CompilerParams(vmem_limit_bytes=1024 * 1024),
    )(fields[0])
    if not tail:
        return out
    piece = math.gcd(length, PIECE_ROWS)
    outer = VMEM((2, length, K, L), dtype)
    fresh = pl.pallas_call(
        functools.partial(tail_kernel, sizes, shape, length, piece),
        out_shape=outer,
        in_specs=[in_vmem] * 3,
        out_specs=in_vmem,
        scratch_shapes=[outer, DMA((2, length // piece)), DMA((2, length // piece))],
        compiler_params=pltpu.CompilerParams(
            collective_id=1, has_side_effects=True, vmem_limit_bytes=4 * 1024 * 1024),
    )(pltpu.with_memory_space_constraint(done, VMEM), *fields)
    return pl.pallas_call(
        functools.partial(patch_kernel, sizes, shape, length, piece),
        out_shape=jax.ShapeDtypeStruct(shape, dtype),
        in_specs=[in_vmem, anywhere],
        out_specs=anywhere,
        scratch_shapes=[DMA((2, length // piece))],
        input_output_aliases={1: 0},
        compiler_params=pltpu.CompilerParams(vmem_limit_bytes=1024 * 1024),
    )(pltpu.with_memory_space_constraint(fresh, VMEM), out)


def solution(mesh):
    spec = P("lat", "lon", "lev", None)
    sizes = tuple(mesh.shape[axis] for axis in AXES)
    return jax.shard_map(
        functools.partial(local, sizes), mesh=mesh, in_specs=(spec, spec), out_specs=spec,
        check_vma=False,
    )
```
